32 devices in a mesh: ctx: 16 (over z, y, core), tp: 2 (over x).
Axes of the slice: x: 2, y: 2, z: 4, core: 2. Of those that a mesh axis runs over, the one named last changes fastest.
Arguments:
- query_se: bfloat16 [3584, 8192], P('ctx', 'tp'), may hold values from -6 to 6
- key_se: bfloat16 [3584, 8192], P('ctx', 'tp'), may hold values from -6 to 6
- value_se: bfloat16 [3584, 8192], P('ctx', 'tp'), may hold values from -6 to 6
- query_mr: bfloat16 [3584, 8192], P('ctx', 'tp'), may hold values from -6 to 6
- key_mr: bfloat16 [3584, 8192], P('ctx', 'tp'), may hold values from -6 to 6
- upstream: bfloat16 [3584, 8192], P('ctx', 'tp'), may hold values from -6 to 6
- filter_se: float32 [7, 8192], P(None, 'tp'), may hold values from -2 to 2
- filter_mr: float32 [128, 8192], P(None, 'tp'), may hold values from -0.5 to 0.5
- skip_mr: float32 [8192], P('tp'), may hold values from -1 to 1
- norm_gain: float32 [8192], P('tp'), may hold values from 0.1 to 1.9
Outputs:
- grad_query_se: bfloat16 [3584, 8192], P('ctx', 'tp')
- grad_key_se: bfloat16 [3584, 8192], P('ctx', 'tp')
- grad_value_se: bfloat16 [3584, 8192], P('ctx', 'tp')
- grad_query_mr: bfloat16 [3584, 8192], P('ctx', 'tp')
- grad_key_mr: bfloat16 [3584, 8192], P('ctx', 'tp')
- grad_filter_se: float32 [7, 8192], P(None, ('tp', 'ctx'))
- grad_filter_mr: float32 [128, 8192], P(None, ('tp', 'ctx'))
- grad_skip: float32 [8192], P(('tp', 'ctx'))
- grad_gain: float32 [8192], P(('tp', 'ctx'))
The draws below stay inside these ranges and needn't reach their ends.
All inputs are finite; a program needn't handle non-finite values.
Results may differ from the reference program's by a relative error of at most 0.0062.
Values may be sent and summed in bfloat16 or wider, within the bound.
A program may use at most 128 MiB of HBM per device.

```python
import math
import jax
import jax.numpy as jnp
from jax import lax

D = 8192
SE_TAPS = 7
MR_TAPS = 128
TOKENS = 3584


def block_scale(rng, dims, split, least, high):
    loudness, own = 1.0, jax.random.fold_in(rng, 6)
    for dim, blocks in split:
        heights = jnp.exp(jax.random.uniform(jax.random.fold_in(own, dim), (blocks,), jnp.float32, least / len(split), high / len(split)))
        loudness = loudness * jnp.repeat(heights, dims[dim] // blocks).reshape([-1 if axis == dim else 1 for axis in range(len(dims))])
    return loudness


def bell_draw(key, extent, scale, limit, pieces=(), kind=jnp.bfloat16):
    loudness = block_scale(key, extent, pieces, -0.22, 0.18) if pieces else 1.0
    drawn = jax.random.normal(key, extent, jnp.float32) * scale * loudness
    return jnp.minimum(jnp.maximum(drawn, -limit), limit).astype(kind)


def setup_inputs(seed: int = 0) -> dict:
    streams_of = jax.random.split(jax.random.key(seed), 11)
    query_se = bell_draw(streams_of[0], (TOKENS, D), 1.0, 6.0, ((0, 16), (1, 2)))
    key_se = bell_draw(streams_of[1], (TOKENS, D), 1.0, 6.0, ((0, 16), (1, 2)))
    value_se = bell_draw(streams_of[2], (TOKENS, D), 1.0, 6.0, ((0, 16), (1, 2)))
    query_mr = bell_draw(streams_of[3], (TOKENS, D), 1.0, 6.0, ((0, 16), (1, 2)))
    key_mr = bell_draw(streams_of[4], (TOKENS, D), 1.0, 6.0, ((0, 16), (1, 2)))
    upstream = bell_draw(streams_of[5], (TOKENS, D), 1.0, 6.0, ((0, 16), (1, 2)))
    filter_se = bell_draw(streams_of[6], (SE_TAPS, D), SE_TAPS ** -0.5, 2.0, ((1, 2),), jnp.float32)
    filter_mr = bell_draw(streams_of[7], (MR_TAPS, D), MR_TAPS ** -0.5, 0.5, ((1, 2),), jnp.float32)
    skip_mr = jnp.clip(jax.random.uniform(streams_of[8], (D,), jnp.float32, -1.0, 1.0) * block_scale(streams_of[8], (D,), ((0, 2),), -0.4, 0.0), -1.0, 1.0)
    norm_gain = jnp.clip(1.0 + 0.18 * jax.random.normal(streams_of[9], (D,), jnp.float32), 0.1, 1.9)
    return {"query_se": query_se, "key_se": key_se, "value_se": value_se, "query_mr": query_mr, "key_mr": key_mr, "upstream": upstream, "filter_se": filter_se, "filter_mr": filter_mr, "skip_mr": skip_mr, "norm_gain": norm_gain}


EPSILON = 0.1

def rounded(value):
    half = lax.optimization_barrier(value.astype(jnp.bfloat16))
    return half.astype(jnp.float32)

def to_blocks(array, width):
    rows, chans = array.shape
    return array.reshape(rows, chans // width, width).transpose(1, 0, 2)

def from_blocks(array):
    count, rows, width = array.shape
    return array.transpose(1, 0, 2).reshape(rows, count * width)

def shift_down(field, steps):
    zeros = jnp.zeros((steps, field.shape[1]), field.dtype)
    return jnp.concatenate([zeros, field[:field.shape[0] - steps]], 0)

def shift_up(field, steps):
    zeros = jnp.zeros((steps, field.shape[1]), field.dtype)
    return jnp.concatenate([field[steps:], zeros], 0)

def short_conv(field, taps):
    result = taps[0] * field
    for step in range(1, taps.shape[0]):
        result = result + taps[step] * shift_down(field, step)
    return result

def short_adjoint(field, taps):
    result = taps[0] * field
    for step in range(1, taps.shape[0]):
        result = result + taps[step] * shift_up(field, step)
    return result

def short_corr(grads, field, count):
    return jnp.stack([lax.optimization_barrier(jnp.sum(grads * shift_down(field, step), axis=0)) for step in range(count)], 0)

def long_conv(field, taps, length):
    spectrum = jnp.fft.rfft(field, n=length, axis=0) * jnp.fft.rfft(taps, n=length, axis=0)
    return jnp.fft.irfft(spectrum, n=length, axis=0)[:field.shape[0]]

def long_adjoint(field, taps, length):
    spectrum = jnp.fft.rfft(field, n=length, axis=0) * jnp.conj(jnp.fft.rfft(taps, n=length, axis=0))
    return jnp.fft.irfft(spectrum, n=length, axis=0)[:field.shape[0]]

def long_corr(grads, field, length, count):
    spectrum = jnp.fft.rfft(grads, n=length, axis=0) * jnp.conj(jnp.fft.rfft(field, n=length, axis=0))
    return jnp.fft.irfft(spectrum, n=length, axis=0)[:count]

def reference(query_se, key_se, value_se, query_mr, key_mr, upstream, filter_se, filter_mr, skip_mr, norm_gain):
    width = math.gcd(D, 1024)
    count = D // width
    length = TOKENS + MR_TAPS
    b_qse = to_blocks(query_se, width)
    b_kse = to_blocks(key_se, width)
    b_vse = to_blocks(value_se, width)
    b_qmr = to_blocks(query_mr, width)
    b_kmr = to_blocks(key_mr, width)
    b_up = to_blocks(upstream, width)
    b_fse = to_blocks(filter_se, width)
    b_fmr = to_blocks(filter_mr, width)
    b_skip = skip_mr.reshape(count, width)
    b_gain = norm_gain.reshape(count, width)

    def short_layer(query, keys, values, taps):
        product = rounded(keys.astype(jnp.float32) * values.astype(jnp.float32))
        conv = short_conv(product, taps)
        return (product, conv, query.astype(jnp.float32) * conv)

    def first(items):
        query, keys, values, taps = items
        product, conv, mixed = short_layer(query, keys, values, taps)
        return lax.optimization_barrier(jnp.sum(mixed * mixed, axis=1))
    squares = lax.optimization_barrier(jnp.sum(lax.map(first, (b_qse, b_kse, b_vse, b_fse)), axis=0))
    scale_rows = lax.rsqrt(squares / D + EPSILON)

    def second(items):
        query, keys, values, taps, gate_q, gate_k, cotan, long_taps, skip, gain = items
        product, conv, mixed = short_layer(query, keys, values, taps)
        normed = mixed * scale_rows[:, None] * gain
        product_mr = rounded(gate_k.astype(jnp.float32) * normed)
        conv_mr = long_conv(product_mr, long_taps, length) + skip * product_mr
        cot = cotan.astype(jnp.float32)
        grad_query_mr = (cot * conv_mr).astype(jnp.bfloat16)
        grad_conv_mr = rounded(cot * gate_q.astype(jnp.float32))
        grad_product_mr = long_adjoint(grad_conv_mr, long_taps, length) + skip * grad_conv_mr
        grad_key_mr = (grad_product_mr * normed).astype(jnp.bfloat16)
        grad_normed = grad_product_mr * gate_k.astype(jnp.float32)
        weighted = lax.optimization_barrier(jnp.sum(grad_normed * gain * mixed, axis=1))
        grad_filter_mr = long_corr(grad_conv_mr, product_mr, length, MR_TAPS)
        grad_skip = lax.optimization_barrier(jnp.sum(grad_conv_mr * product_mr, axis=0))
        grad_gain = lax.optimization_barrier(jnp.sum(grad_normed * mixed * scale_rows[:, None], axis=0))
        return (grad_query_mr, grad_key_mr, grad_normed, weighted, grad_filter_mr, grad_skip, grad_gain)
    out_b = lax.map(second, (b_qse, b_kse, b_vse, b_fse, b_qmr, b_kmr, b_up, b_fmr, b_skip, b_gain))
    grad_query_mr, grad_key_mr, grad_normed, weighted, grad_filter_mr, grad_skip, grad_gain = out_b
    weighted = lax.optimization_barrier(jnp.sum(weighted, axis=0))

    def third(items):
        query, keys, values, taps, gain, back = items
        product, conv, mixed = short_layer(query, keys, values, taps)
        grad_mixed = gain * scale_rows[:, None] * back - mixed * (scale_rows ** 3 * weighted / D)[:, None]
        grad_query_se = (grad_mixed * conv).astype(jnp.bfloat16)
        grad_conv_se = rounded(grad_mixed * query.astype(jnp.float32))
        grad_product_se = short_adjoint(grad_conv_se, taps)
        grad_key_se = (grad_product_se * values.astype(jnp.float32)).astype(jnp.bfloat16)
        grad_value_se = (grad_product_se * keys.astype(jnp.float32)).astype(jnp.bfloat16)
        grad_filter_se = short_corr(grad_conv_se, product, SE_TAPS)
        return (grad_query_se, grad_key_se, grad_value_se, grad_filter_se)
    grad_query_se, grad_key_se, grad_value_se, grad_filter_se = lax.map(third, (b_qse, b_kse, b_vse, b_fse, b_gain, grad_normed))
    factor = 1.0 / math.sqrt(TOKENS)
    return (from_blocks(grad_query_se), from_blocks(grad_key_se), from_blocks(grad_value_se), from_blocks(grad_query_mr), from_blocks(grad_key_mr), from_blocks(grad_filter_se) * factor, from_blocks(grad_filter_mr) * factor, grad_skip.reshape(D) * factor, grad_gain.reshape(D) * factor)
```

```python
import functools
import math

import jax
import jax.numpy as jnp
import numpy as np
from jax import lax
from jax.experimental import pallas as pl
from jax.experimental.pallas import tpu as pltpu
from jax.sharding import PartitionSpec as P

EPSILON = 0.1
F32 = jnp.float32
BF16 = jnp.bfloat16
LANES = 128


def shifted(block, axis, distance):
    devices = range(lax.axis_size(axis))
    route = [(i - distance, i) for i in devices if i - distance in devices]
    return lax.ppermute(block, axis, route)


def transforms(rows, taps):
    length = rows + taps
    freq = 2.0 * np.pi * (np.arange(length // 2) + 0.5) / length

    def forward(start, stop):
        angle = freq[:, None] * np.arange(start, stop)[None, :]
        return np.concatenate([np.cos(angle), -np.sin(angle)], 0)

    angle = np.arange(max(rows, taps))[:, None] * freq[None, :]
    inverse = np.concatenate([np.cos(angle), -np.sin(angle)], 1) * (2.0 / length)
    mats = forward(-taps, rows), forward(0, length), forward(0, taps), inverse
    return [jnp.asarray(m, BF16) for m in mats]


def dot(a, b):
    return jnp.dot(a, b, preferred_element_type=F32)


def lane_sum(value):
    total = value[:, :LANES]
    for start in range(LANES, value.shape[1], LANES):
        total = total + value[:, start : start + LANES]
    return total


def row_scale(width, *parts):
    total = parts[0][...]
    for part in parts[1:]:
        total = total + part[...]
    return lax.rsqrt(jnp.sum(total, axis=1, keepdims=True) * (1.0 / width) + EPSILON)


def short_kernel(q_ref, k_ref, v_ref, tail_ref, f_ref, conv_ref, sq_ref, pad):
    rows, block = q_ref.shape
    halo = tail_ref.shape[0]

    @pl.when(pl.program_id(0) == 0)
    def _():
        sq_ref[...] = jnp.zeros_like(sq_ref)

    for start in range(0, block, LANES):
        cols = slice(start, start + LANES)
        pad[:halo, :] = tail_ref[:, cols].astype(F32)
        product = k_ref[:, cols].astype(F32) * v_ref[:, cols].astype(F32)
        pad[halo:, :] = product.astype(BF16).astype(F32)
        conv = f_ref[0:1, cols] * pad[pl.ds(halo, rows), :]
        for j in range(1, f_ref.shape[0]):
            conv = conv + f_ref[j : j + 1, cols] * pad[pl.ds(halo - j, rows), :]
        conv_ref[:, cols] = conv
        mixed = q_ref[:, cols].astype(F32) * conv
        sq_ref[...] += mixed * mixed


def product_kernel(width, nsq, *refs):
    sq = refs[:nsq]
    q_ref, conv_ref, km_ref, gain_ref, out_ref, tail_ref = refs[nsq:]
    scale = row_scale(width, *sq)
    halo = tail_ref.shape[0]
    for start in range(0, q_ref.shape[1], LANES):
        cols = slice(start, start + LANES)
        normed = q_ref[:, cols].astype(F32) * conv_ref[:, cols] * scale * gain_ref[:, cols]
        product = (km_ref[:, cols].astype(F32) * normed).astype(BF16)
        out_ref[:, cols] = product
        tail_ref[:, cols] = product[product.shape[0] - halo :]


def adjoint_kernel(width, nsq, *refs):
    sq = refs[:nsq]
    (up_ref, qm_ref, head_ref, f_ref, skip_ref, q_ref, conv_ref, km_ref, gain_ref,
     fg_ref, fh_ref, inv_ref, gk_ref, gn_ref, w_ref) = refs[nsq:]
    rows, block = q_ref.shape
    half = fg_ref.shape[0] // 2

    @pl.when(pl.program_id(0) == 0)
    def _():
        w_ref[...] = jnp.zeros_like(w_ref)

    g = (up_ref[...].astype(F32) * qm_ref[...].astype(F32)).astype(BF16)
    gs = dot(fg_ref[...], jnp.concatenate([g, head_ref[...]], 0))
    hs = dot(fh_ref[...], f_ref[...].astype(BF16))
    hr, hi = hs[:half] + skip_ref[...], hs[half:]
    gr, gi = gs[:half], gs[half:]
    spectrum = jnp.concatenate(
        [(gr * hr + gi * hi).astype(BF16), (gi * hr - gr * hi).astype(BF16)], 0
    )
    gp = dot(inv_ref[:rows, :], spectrum)
    scale = row_scale(width, *sq)
    for start in range(0, block, LANES):
        cols = slice(start, start + LANES)
        mixed = q_ref[:, cols].astype(F32) * conv_ref[:, cols]
        back = gp[:, cols]
        gain = gain_ref[:, cols]
        gk_ref[:, cols] = (back * (mixed * scale * gain)).astype(BF16)
        gn = back * km_ref[:, cols].astype(F32)
        gn_ref[:, cols] = gn
        w_ref[...] += gn * gain * mixed


def medium_kernel(z_ref, tail_ref, up_ref, qm_ref, f_ref, skip_ref, fz_ref, fg_ref, fh_ref,
                  inv_ref, gq_ref, corr_ref):
    rows, block = up_ref.shape
    half = fz_ref.shape[0] // 2
    taps = f_ref.shape[0]
    up = up_ref[...].astype(F32)
    g = (up * qm_ref[...].astype(F32)).astype(BF16)
    zs = dot(fz_ref[...], jnp.concatenate([tail_ref[...], z_ref[...]], 0))
    hs = dot(fh_ref[...], f_ref[...].astype(BF16))
    gs = dot(fg_ref[:, :rows], g)
    hr, hi = hs[:half] + skip_ref[...], hs[half:]
    zr, zi = zs[:half], zs[half:]
    gr, gi = gs[:half], gs[half:]
    spectrum = jnp.concatenate(
        [(zr * hr - zi * hi).astype(BF16), (zr * hi + zi * hr).astype(BF16)], 0
    )
    gq_ref[...] = (up * dot(inv_ref[:rows, :], spectrum)).astype(BF16)
    cross = jnp.concatenate(
        [(gr * zr + gi * zi).astype(BF16), (gi * zr - gr * zi).astype(BF16)], 0
    )
    corr = dot(inv_ref[:taps, :], cross)
    share = corr_ref.shape[2]
    for part in range(corr_ref.shape[0]):
        corr_ref[part] = corr[:, part * share : (part + 1) * share]


def back_kernel(width, nsq, *refs):
    sq, ws = refs[:nsq], refs[nsq : 2 * nsq]
    (q_ref, k_ref, v_ref, tail_ref, head_ref, conv_ref, gn_ref, gain_ref, f_ref,
     gq_ref, gk_ref, gv_ref, small_ref, pad_p, pad_g) = refs[2 * nsq :]
    rows, block = q_ref.shape
    halo = tail_ref.shape[0]
    taps = f_ref.shape[0]
    share = small_ref.shape[2]
    scale = row_scale(width, *sq)
    weight = ws[0][...]
    for part in ws[1:]:
        weight = weight + part[...]
    coef = jnp.sum(weight, axis=1, keepdims=True) * (scale * scale * scale) * (1.0 / width)
    for start in range(0, block, LANES):
        cols = slice(start, start + LANES)
        q = q_ref[:, cols].astype(F32)
        conv = conv_ref[:, cols]
        mixed = q * conv
        gn = gn_ref[:, cols] * scale
        gm = gain_ref[:, cols] * gn - mixed * coef
        gq_ref[:, cols] = (gm * conv).astype(BF16)
        gc = (gm * q).astype(BF16).astype(F32)
        pad_g[:rows, :] = gc
        pad_g[rows:, :] = head_ref[:, cols].astype(F32)
        part, inner = start // share, start % share
        place = slice(inner, inner + LANES)
        small_ref[part, taps : taps + 1, place] = jnp.sum(gn * mixed, axis=0, keepdims=True)
        k = k_ref[:, cols].astype(F32)
        v = v_ref[:, cols].astype(F32)
        pad_p[:halo, :] = tail_ref[:, cols].astype(F32)
        pad_p[halo:, :] = (k * v).astype(BF16).astype(F32)
        gp = f_ref[0:1, cols] * gc
        for j in range(taps):
            if j:
                gp = gp + f_ref[j : j + 1, cols] * pad_g[pl.ds(j, rows), :]
            small_ref[part, j : j + 1, place] = jnp.sum(
                gc * pad_p[pl.ds(halo - j, rows), :], axis=0, keepdims=True
            )
        gk_ref[:, cols] = (gp * v).astype(BF16)
        gv_ref[:, cols] = (gp * k).astype(BF16)


def up_to(value, step):
    return -(-value // step) * step


def split_parts(parts, share):
    count, height, group = parts.shape
    if group == share:
        return parts
    parts = parts.reshape(count, height, group // share, share)
    return parts.transpose(0, 2, 1, 3).reshape(-1, height, share)


def scatter_sum(parts, axis):
    size = lax.axis_size(axis)
    me = lax.axis_index(axis)
    bit = 1
    while bit < size:
        rest = parts.reshape((parts.shape[0] // 2, 2) + parts.shape[1:])
        mine = lax.rem(me // bit, 2)
        away = lax.dynamic_index_in_dim(rest, 1 - mine, 1, keepdims=False).astype(BF16)
        keep = lax.dynamic_index_in_dim(rest, mine, 1, keepdims=False)
        got = lax.ppermute(away, axis, [(i, i ^ bit) for i in range(size)])
        parts = keep + got.astype(F32)
        bit *= 2
    return parts[0]


def exchanged(value, axis):
    size = lax.axis_size(axis)
    others = []
    for step in range(1, size):
        others.append(lax.ppermute(value, axis, [(i, (i + step) % size) for i in range(size)]))
    return [value] + others


def local(
    query_se, key_se, value_se, query_mr, key_mr, upstream, filter_se, filter_mr, skip_mr, norm_gain
):
    rows, chans = query_se.shape
    taps_se, taps = filter_se.shape[0], filter_mr.shape[0]
    ctx = lax.axis_size("ctx")
    width = chans * lax.axis_size("tp")
    tokens = rows * ctx
    share = chans // ctx
    group = up_to(share, LANES)
    halo = up_to(taps_se - 1, 16)
    block = max(group, min(512, chans))
    steps = chans // block
    fz, fg, fh, inv = transforms(rows, taps)
    length = rows + taps
    skip = skip_mr[None]
    gain = norm_gain[None]

    def rowed(n):
        return pl.BlockSpec((n, block), lambda i: (0, i))

    def whole(a):
        return pl.BlockSpec(a.shape, lambda i: (0, 0))

    lanes_spec = pl.BlockSpec((rows, LANES), lambda i: (0, 0))
    stream = rowed(rows)
    one = rowed(1)

    def call(body, name, ins, specs, outs, out_specs, scratch=(), flops=0):
        moved = sum(a.size * a.dtype.itemsize for a in list(ins) + list(outs))
        return pl.pallas_call(
            body,
            name=name,
            grid=(steps,),
            in_specs=specs,
            out_specs=out_specs,
            out_shape=outs,
            scratch_shapes=scratch,
            cost_estimate=pl.CostEstimate(flops=flops, bytes_accessed=moved, transcendentals=0),
            compiler_params=pltpu.CompilerParams(
                dimension_semantics=("arbitrary",), vmem_limit_bytes=56 * 2**20
            ),
        )(*ins)

    def shape(n, kind):
        return jax.ShapeDtypeStruct((n, chans), kind)

    lanes_shape = jax.ShapeDtypeStruct((rows, LANES), F32)

    tail_se = shifted(
        (key_se[rows - halo :].astype(F32) * value_se[rows - halo :].astype(F32)).astype(BF16),
        "ctx", 1,
    )
    head_mr = shifted(
        (upstream[:taps].astype(F32) * query_mr[:taps].astype(F32)).astype(BF16), "ctx", -1
    )
    conv_se, squares = call(
        short_kernel, "short",
        (query_se, key_se, value_se, tail_se, filter_se),
        [stream, stream, stream, rowed(halo), rowed(taps_se)],
        [shape(rows, F32), lanes_shape], [stream, lanes_spec],
        [pltpu.VMEM((halo + rows, LANES), F32)],
    )
    sq = exchanged(squares, "tp")
    nsq = len(sq)
    product_mr, tail = call(
        functools.partial(product_kernel, width, nsq), "product",
        (*sq, query_se, conv_se, key_mr, gain),
        [lanes_spec] * nsq + [stream, stream, stream, one],
        [shape(rows, BF16), shape(taps, BF16)], [stream, rowed(taps)],
    )
    tail_mr = shifted(tail, "ctx", 1)
    grad_key_mr, grad_normed, weight = call(
        functools.partial(adjoint_kernel, width, nsq), "adjoint",
        (*sq, upstream, query_mr, head_mr, filter_mr, skip, query_se, conv_se, key_mr, gain,
         fg, fh, inv),
        [lanes_spec] * nsq
        + [stream, stream, rowed(taps), rowed(taps), one, stream, stream, stream, one,
           whole(fg), whole(fh), whole(inv)],
        [shape(rows, BF16), shape(rows, F32), lanes_shape], [stream, stream, lanes_spec],
        flops=2 * length * (length + taps + rows) * chans,
    )
    ws = exchanged(weight, "tp")
    first = slice(0, halo)
    scale = lax.rsqrt(jnp.sum(sum(a[first] for a in sq), axis=1, keepdims=True) / width + EPSILON)
    coef = scale**3 * jnp.sum(sum(a[first] for a in ws), axis=1, keepdims=True) / width
    q_head = query_se[first].astype(F32)
    mixed_head = gain * scale * grad_normed[first] - q_head * conv_se[first] * coef
    head_se = shifted((mixed_head * q_head).astype(BF16), "ctx", -1)
    grad_query_mr, corr = call(
        medium_kernel, "medium",
        (product_mr, tail_mr, upstream, query_mr, filter_mr, skip, fz, fg, fh, inv),
        [stream, rowed(taps), stream, stream, rowed(taps), one,
         whole(fz), whole(fg), whole(fh), whole(inv)],
        [shape(rows, BF16), jax.ShapeDtypeStruct((chans // group, taps, group), F32)],
        [stream, pl.BlockSpec((block // group, taps, group), lambda i: (i, 0, 0))],
        flops=2 * length * (length + taps + rows + rows + taps) * chans,
    )
    grad_query_se, grad_key_se, grad_value_se, small = call(
        functools.partial(back_kernel, width, nsq), "back",
        (*sq, *ws, query_se, key_se, value_se, tail_se, head_se, conv_se, grad_normed, gain,
         filter_se),
        [lanes_spec] * (2 * nsq)
        + [stream, stream, stream, rowed(halo), rowed(halo), stream, stream, one, rowed(taps_se)],
        [shape(rows, BF16)] * 3 + [jax.ShapeDtypeStruct((chans // group, taps_se + 1, group), F32)],
        [stream] * 3 + [pl.BlockSpec((block // group, taps_se + 1, group), lambda i: (i, 0, 0))],
        [pltpu.VMEM((halo + rows, LANES), F32), pltpu.VMEM((halo + rows, LANES), F32)],
    )
    factor = 1.0 / math.sqrt(tokens)
    corr, small = split_parts(corr, share), split_parts(small, share)
    total_mr = scatter_sum(corr, "ctx") * factor
    total = jnp.sum(lax.all_to_all(small, "ctx", 0, 0, tiled=True), axis=0) * factor
    return (
        grad_query_se,
        grad_key_se,
        grad_value_se,
        grad_query_mr,
        grad_key_mr,
        total[:taps_se],
        total_mr,
        total_mr[0],
        total[taps_se],
    )


def solution(mesh):
    streams = (P("ctx", "tp"),)
    in_specs = streams * 6 + (P(None, "tp"), P(None, "tp"), P("tp"), P("tp"))
    both = ("tp", "ctx")
    out_specs = streams * 5 + (P(None, both), P(None, both), P(both), P(both))
    return jax.shard_map(local, mesh=mesh, in_specs=in_specs, out_specs=out_specs, check_vma=False)
```

```python
import functools
import math

import jax
import jax.numpy as jnp
import numpy as np
from jax import lax
from jax.experimental import pallas as pl
from jax.experimental.pallas import tpu as pltpu
from jax.sharding import PartitionSpec as P


EPSILON = 0.1
F32 = jnp.float32
BF16 = jnp.bfloat16
LANES = 128


def shifted(block, axis, distance):
    devices = range(lax.axis_size(axis))
    route = [(i - distance, i) for i in devices if i - distance in devices]
    return lax.ppermute(block, axis, route)


def transforms(rows, taps):
    length = rows + taps
    freq = 2.0 * np.pi * (np.arange(length // 2) + 0.5) / length

    def forward(start, stop):
        angle = freq[:, None] * np.arange(start, stop)[None, :]
        return np.concatenate([np.cos(angle), -np.sin(angle)], 0)

    angle = np.arange(max(rows, taps))[:, None] * freq[None, :]
    inverse = np.concatenate([np.cos(angle), -np.sin(angle)], 1) * (2.0 / length)
    mats = forward(-taps, rows), forward(0, length), forward(0, taps), inverse
    return [jnp.asarray(m, BF16) for m in mats]


def dot(a, b):
    return jnp.dot(a, b, preferred_element_type=F32)


def row_scale(width, *parts):
    total = parts[0][...]
    for part in parts[1:]:
        total = total + part[...]
    return lax.rsqrt(jnp.sum(total, axis=1, keepdims=True) * (1.0 / width) + EPSILON)


def short_kernel(q_ref, k_ref, v_ref, tail_ref, f_ref, conv_ref, sq_ref, pad):
    rows, block = q_ref.shape
    halo = tail_ref.shape[0]

    @pl.when(pl.program_id(0) == 0)
    def _():
        sq_ref[...] = jnp.zeros_like(sq_ref)

    for start in range(0, block, LANES):
        cols = slice(start, start + LANES)
        pad[:halo, :] = tail_ref[:, cols].astype(F32)
        product = k_ref[:, cols].astype(F32) * v_ref[:, cols].astype(F32)
        pad[halo:, :] = product.astype(BF16).astype(F32)
        conv = f_ref[0:1, cols] * pad[pl.ds(halo, rows), :]
        for j in range(1, f_ref.shape[0]):
            conv = conv + f_ref[j : j + 1, cols] * pad[pl.ds(halo - j, rows), :]
        conv_ref[:, cols] = conv
        mixed = q_ref[:, cols].astype(F32) * conv
        sq_ref[...] += mixed * mixed


def spectrum_of(real, imag):
    return jnp.concatenate([real.astype(BF16), imag.astype(BF16)], 0)


def adjoint_kernel(width, nsq, *refs):
    sq = refs[:nsq]
    (up_ref, qm_ref, head_ref, f_ref, skip_ref, q_ref, conv_ref, km_ref, gain_ref,
     fg_ref, fh_ref, inv_ref, gk_ref, gn_ref, w_ref, z_ref, tail_ref, corr_ref,
     scale_ref) = refs[nsq:]
    rows, block = q_ref.shape
    taps = f_ref.shape[0]
    half = fg_ref.shape[0] // 2

    @pl.when(pl.program_id(0) == 0)
    def _():
        w_ref[...] = jnp.zeros_like(w_ref)
        scale_ref[...] = jnp.broadcast_to(row_scale(width, *sq), scale_ref.shape)

    g = (up_ref[...].astype(F32) * qm_ref[...].astype(F32)).astype(BF16)
    gs = dot(fg_ref[...], jnp.concatenate([g, head_ref[...]], 0))
    hs = dot(fh_ref[...], f_ref[...].astype(BF16))
    hr, hi = hs[:half] + skip_ref[...], hs[half:]
    gr, gi = gs[:half], gs[half:]
    gp = dot(inv_ref[:rows, :], spectrum_of(gr * hr + gi * hi, gi * hr - gr * hi))
    scale = scale_ref[...]
    for start in range(0, block, LANES):
        cols = slice(start, start + LANES)
        mixed = q_ref[:, cols].astype(F32) * conv_ref[:, cols]
        back = gp[:, cols]
        gain = gain_ref[:, cols]
        km = km_ref[:, cols].astype(F32)
        normed = mixed * scale * gain
        gk_ref[:, cols] = (back * normed).astype(BF16)
        z_ref[:, cols] = (km * normed).astype(BF16)
        gn = back * km
        gn_ref[:, cols] = gn
        w_ref[...] += gn * gain * mixed
    tail_ref[...] = z_ref[rows - taps :, :]
    zs = dot(fg_ref[:, :rows], z_ref[...])
    zr, zi = zs[:half], zs[half:]
    corr = dot(inv_ref[:taps, :], spectrum_of(gr * zr + gi * zi, gi * zr - gr * zi))
    share = corr_ref.shape[2]
    for part in range(corr_ref.shape[0]):
        corr_ref[part] = corr[:, part * share : (part + 1) * share]


def medium_kernel(z_ref, tail_ref, up_ref, f_ref, skip_ref, fz_ref, fh_ref, inv_ref, gq_ref):
    rows, _ = up_ref.shape
    half = fz_ref.shape[0] // 2
    zs = dot(fz_ref[...], jnp.concatenate([tail_ref[...], z_ref[...]], 0))
    hs = dot(fh_ref[...], f_ref[...].astype(BF16))
    hr, hi = hs[:half] + skip_ref[...], hs[half:]
    zr, zi = zs[:half], zs[half:]
    conv = dot(inv_ref[:rows, :], spectrum_of(zr * hr - zi * hi, zr * hi + zi * hr))
    gq_ref[...] = (up_ref[...].astype(F32) * conv).astype(BF16)


def back_kernel(width, nsq, *refs):
    sq, ws = refs[:nsq], refs[nsq : 2 * nsq]
    (q_ref, k_ref, v_ref, tail_ref, head_ref, conv_ref, gn_ref, gain_ref, f_ref,
     gq_ref, gk_ref, gv_ref, small_ref, pad_p, pad_g, scale_ref, coef_ref) = refs[2 * nsq :]
    rows, block = q_ref.shape
    halo = tail_ref.shape[0]
    taps = f_ref.shape[0]
    share = small_ref.shape[2]

    @pl.when(pl.program_id(0) == 0)
    def _():
        scale = row_scale(width, *sq)
        weight = ws[0][...]
        for part in ws[1:]:
            weight = weight + part[...]
        coef = jnp.sum(weight, axis=1, keepdims=True) * (scale * scale * scale) * (1.0 / width)
        scale_ref[...] = jnp.broadcast_to(scale, scale_ref.shape)
        coef_ref[...] = jnp.broadcast_to(coef, coef_ref.shape)

    scale, coef = scale_ref[...], coef_ref[...]
    for start in range(0, block, LANES):
        cols = slice(start, start + LANES)
        q = q_ref[:, cols].astype(F32)
        conv = conv_ref[:, cols]
        mixed = q * conv
        gn = gn_ref[:, cols] * scale
        gm = gain_ref[:, cols] * gn - mixed * coef
        gq_ref[:, cols] = (gm * conv).astype(BF16)
        gc = (gm * q).astype(BF16).astype(F32)
        pad_g[:rows, :] = gc
        pad_g[rows:, :] = head_ref[:, cols].astype(F32)
        part, inner = start // share, start % share
        place = slice(inner, inner + LANES)
        small_ref[part, taps : taps + 1, place] = jnp.sum(gn * mixed, axis=0, keepdims=True)
        k = k_ref[:, cols].astype(F32)
        v = v_ref[:, cols].astype(F32)
        pad_p[:halo, :] = tail_ref[:, cols].astype(F32)
        pad_p[halo:, :] = (k * v).astype(BF16).astype(F32)
        gp = f_ref[0:1, cols] * gc
        for j in range(taps):
            if j:
                gp = gp + f_ref[j : j + 1, cols] * pad_g[pl.ds(j, rows), :]
            small_ref[part, j : j + 1, place] = jnp.sum(
                gc * pad_p[pl.ds(halo - j, rows), :], axis=0, keepdims=True
            )
        gk_ref[:, cols] = (gp * v).astype(BF16)
        gv_ref[:, cols] = (gp * k).astype(BF16)


def up_to(value, step):
    return -(-value // step) * step


def split_parts(parts, share):
    count, height, group = parts.shape
    if group == share:
        return parts
    parts = parts.reshape(count, height, group // share, share)
    return parts.transpose(0, 2, 1, 3).reshape(-1, height, share)


def scatter_sum(parts, axis):
    size = lax.axis_size(axis)
    me = lax.axis_index(axis)
    bit = 1
    while bit < size:
        rest = parts.reshape((parts.shape[0] // 2, 2) + parts.shape[1:])
        mine = lax.rem(me // bit, 2)
        away = lax.dynamic_index_in_dim(rest, 1 - mine, 1, keepdims=False).astype(BF16)
        keep = lax.dynamic_index_in_dim(rest, mine, 1, keepdims=False)
        got = lax.ppermute(away, axis, [(i, i ^ bit) for i in range(size)])
        parts = keep + got.astype(F32)
        bit *= 2
    return parts[0]


def exchanged(value, axis):
    size = lax.axis_size(axis)
    others = []
    for step in range(1, size):
        others.append(lax.ppermute(value, axis, [(i, (i + step) % size) for i in range(size)]))
    return [value] + others


def local(
    query_se, key_se, value_se, query_mr, key_mr, upstream, filter_se, filter_mr, skip_mr, norm_gain
):
    rows, chans = query_se.shape
    taps_se, taps = filter_se.shape[0], filter_mr.shape[0]
    ctx = lax.axis_size("ctx")
    width = chans * lax.axis_size("tp")
    tokens = rows * ctx
    share = chans // ctx
    group = up_to(share, LANES)
    halo = up_to(taps_se - 1, 16)
    block = max(group, min(512, chans))
    steps = chans // block
    fz, fg, fh, inv = transforms(rows, taps)
    length = rows + taps
    skip = skip_mr[None]
    gain = norm_gain[None]

    def rowed(n):
        return pl.BlockSpec((n, block), lambda i: (0, i))

    def whole(a):
        return pl.BlockSpec(a.shape, lambda i: (0, 0))

    lanes_spec = pl.BlockSpec((rows, LANES), lambda i: (0, 0))
    stream = rowed(rows)
    one = rowed(1)

    def call(body, ins, specs, outs, out_specs, scratch=(), flops=0):
        moved = sum(a.size * a.dtype.itemsize for a in list(ins) + list(outs))
        return pl.pallas_call(
            body,
            grid=(steps,),
            in_specs=specs,
            out_specs=out_specs,
            out_shape=outs,
            scratch_shapes=scratch,
            cost_estimate=pl.CostEstimate(flops=flops, bytes_accessed=moved, transcendentals=0),
            compiler_params=pltpu.CompilerParams(
                dimension_semantics=("arbitrary",), vmem_limit_bytes=58 * 2**20
            ),
        )(*ins)

    def shape(n, kind):
        return jax.ShapeDtypeStruct((n, chans), kind)

    lanes_shape = jax.ShapeDtypeStruct((rows, LANES), F32)

    tail_se = shifted(
        (key_se[rows - halo :].astype(F32) * value_se[rows - halo :].astype(F32)).astype(BF16),
        "ctx", 1,
    )
    head_mr = shifted(
        (upstream[:taps].astype(F32) * query_mr[:taps].astype(F32)).astype(BF16), "ctx", -1
    )
    conv_se, squares = call(
        short_kernel,
        (query_se, key_se, value_se, tail_se, filter_se),
        [stream, stream, stream, rowed(halo), rowed(taps_se)],
        [shape(rows, F32), lanes_shape], [stream, lanes_spec],
        [pltpu.VMEM((halo + rows, LANES), F32)],
    )
    sq = exchanged(squares, "tp")
    nsq = len(sq)
    group_spec = pl.BlockSpec((block // group, taps, group), lambda i: (i, 0, 0))
    grad_key_mr, grad_normed, weight, product_mr, tail, corr = call(
        functools.partial(adjoint_kernel, width, nsq),
        (*sq, upstream, query_mr, head_mr, filter_mr, skip, query_se, conv_se, key_mr, gain,
         fg, fh, inv),
        [lanes_spec] * nsq
        + [stream, stream, rowed(taps), rowed(taps), one, stream, stream, stream, one,
           whole(fg), whole(fh), whole(inv)],
        [shape(rows, BF16), shape(rows, F32), lanes_shape, shape(rows, BF16),
         shape(taps, BF16), jax.ShapeDtypeStruct((chans // group, taps, group), F32)],
        [stream, stream, lanes_spec, stream, rowed(taps), group_spec],
        [pltpu.VMEM((rows, LANES), F32)],
        flops=2 * length * (length + taps + 2 * rows + taps) * chans,
    )
    tail_mr = shifted(tail, "ctx", 1)
    ws = exchanged(weight, "tp")
    first = slice(0, halo)
    scale = lax.rsqrt(jnp.sum(sum(a[first] for a in sq), axis=1, keepdims=True) / width + EPSILON)
    coef = scale**3 * jnp.sum(sum(a[first] for a in ws), axis=1, keepdims=True) / width
    q_head = query_se[first].astype(F32)
    mixed_head = gain * scale * grad_normed[first] - q_head * conv_se[first] * coef
    head_se = shifted((mixed_head * q_head).astype(BF16), "ctx", -1)
    grad_query_se, grad_key_se, grad_value_se, small = call(
        functools.partial(back_kernel, width, nsq),
        (*sq, *ws, query_se, key_se, value_se, tail_se, head_se, conv_se, grad_normed, gain,
         filter_se),
        [lanes_spec] * (2 * nsq)
        + [stream, stream, stream, rowed(halo), rowed(halo), stream, stream, one, rowed(taps_se)],
        [shape(rows, BF16)] * 3 + [jax.ShapeDtypeStruct((chans // group, taps_se + 1, group), F32)],
        [stream] * 3 + [pl.BlockSpec((block // group, taps_se + 1, group), lambda i: (i, 0, 0))],
        [pltpu.VMEM((halo + rows, LANES), F32)] * 2 + [pltpu.VMEM((rows, LANES), F32)] * 2,
    )
    corr, small = split_parts(corr, share), split_parts(small, share)
    small = lax.all_to_all(small, "ctx", 0, 0, tiled=True)
    (grad_query_mr,) = call(
        medium_kernel,
        (product_mr, tail_mr, upstream, filter_mr, skip, fz, fh, inv),
        [stream, rowed(taps), stream, rowed(taps), one, whole(fz), whole(fh), whole(inv)],
        [shape(rows, BF16)], [stream],
        flops=2 * length * (length + taps + rows) * chans,
    )
    factor = 1.0 / math.sqrt(tokens)
    total_mr = scatter_sum(corr, "ctx") * factor
    total = jnp.sum(small, axis=0) * factor
    return (
        grad_query_se,
        grad_key_se,
        grad_value_se,
        grad_query_mr,
        grad_key_mr,
        total[:taps_se],
        total_mr,
        total_mr[0],
        total[taps_se],
    )


def solution(mesh):
    streams = (P("ctx", "tp"),)
    in_specs = streams * 6 + (P(None, "tp"), P(None, "tp"), P("tp"), P("tp"))
    both = ("tp", "ctx")
    out_specs = streams * 5 + (P(None, both), P(None, both), P(both), P(both))

    return jax.shard_map(local, mesh=mesh, in_specs=in_specs, out_specs=out_specs, check_vma=False)
```

```python
import functools
import math

import jax
import jax.numpy as jnp
import numpy as np
from jax import lax
from jax.experimental import pallas as pl
from jax.experimental.pallas import tpu as pltpu
from jax.sharding import PartitionSpec as P


EPSILON = 0.1
F32 = jnp.float32
BF16 = jnp.bfloat16
LANES = 128


def shifted(block, axis, distance):
    devices = range(lax.axis_size(axis))
    route = [(i - distance, i) for i in devices if i - distance in devices]
    return lax.ppermute(block, axis, route)


def transforms(rows, taps):
    length = rows + taps
    freq = 2.0 * np.pi * (np.arange(length // 2) + 0.5) / length

    def forward(start, stop):
        angle = freq[:, None] * np.arange(start, stop)[None, :]
        return np.concatenate([np.cos(angle), -np.sin(angle)], 0)

    angle = np.arange(max(rows, taps))[:, None] * freq[None, :]
    inverse = np.concatenate([np.cos(angle), -np.sin(angle)], 1) * (2.0 / length)
    mats = forward(-taps, rows), forward(0, length), forward(0, taps), inverse
    return [jnp.asarray(m, BF16) for m in mats]


def dot(a, b):
    return jnp.dot(a, b, preferred_element_type=F32)


def row_scale(width, *parts):
    total = parts[0][...]
    for part in parts[1:]:
        total = total + part[...]
    return lax.rsqrt(jnp.sum(total, axis=1, keepdims=True) * (1.0 / width) + EPSILON)


def short_kernel(q_ref, k_ref, v_ref, tail_ref, f_ref, conv_ref, sq_ref, pad):
    rows, block = q_ref.shape
    halo = tail_ref.shape[0]

    @pl.when(pl.program_id(0) == 0)
    def _():
        sq_ref[...] = jnp.zeros_like(sq_ref)

    for start in range(0, block, LANES):
        cols = slice(start, start + LANES)
        pad[:halo, :] = tail_ref[:, cols].astype(F32)
        product = k_ref[:, cols].astype(F32) * v_ref[:, cols].astype(F32)
        pad[halo:, :] = product.astype(BF16).astype(F32)
        conv = f_ref[0:1, cols] * pad[pl.ds(halo, rows), :]
        for j in range(1, f_ref.shape[0]):
            conv = conv + f_ref[j : j + 1, cols] * pad[pl.ds(halo - j, rows), :]
        conv_ref[:, cols] = conv
        mixed = q_ref[:, cols].astype(F32) * conv
        sq_ref[...] += mixed * mixed


def spectrum_of(real, imag):
    return jnp.concatenate([real.astype(BF16), imag.astype(BF16)], 0)


def adjoint_kernel(width, nsq, *refs):
    sq = refs[:nsq]
    (up_ref, qm_ref, head_ref, f_ref, skip_ref, q_ref, conv_ref, km_ref, gain_ref,
     fg_ref, fh_ref, inv_ref, gk_ref, gn_ref, w_ref, z_ref, tail_ref, corr_ref,
     scale_ref) = refs[nsq:]
    rows, block = q_ref.shape
    taps = f_ref.shape[0]
    half = fg_ref.shape[0] // 2

    @pl.when(pl.program_id(0) == 0)
    def _():
        w_ref[...] = jnp.zeros_like(w_ref)
        scale_ref[...] = jnp.broadcast_to(row_scale(width, *sq), scale_ref.shape)

    g = (up_ref[...].astype(F32) * qm_ref[...].astype(F32)).astype(BF16)
    gs = dot(fg_ref[...], jnp.concatenate([g, head_ref[...]], 0))
    hs = dot(fh_ref[...], f_ref[...].astype(BF16))
    hr, hi = hs[:half] + skip_ref[...], hs[half:]
    gr, gi = gs[:half], gs[half:]
    gp = dot(inv_ref[:rows, :], spectrum_of(gr * hr + gi * hi, gi * hr - gr * hi))
    scale = scale_ref[...]
    for start in range(0, block, LANES):
        cols = slice(start, start + LANES)
        mixed = q_ref[:, cols].astype(F32) * conv_ref[:, cols]
        back = gp[:, cols]
        gain = gain_ref[:, cols]
        km = km_ref[:, cols].astype(F32)
        normed = mixed * scale * gain
        gk_ref[:, cols] = (back * normed).astype(BF16)
        z_ref[:, cols] = (km * normed).astype(BF16)
        gn = back * km
        gn_ref[:, cols] = gn
        w_ref[...] += gn * gain * mixed
    tail_ref[...] = z_ref[rows - taps :, :]
    zs = dot(fg_ref[:, :rows], z_ref[...])
    zr, zi = zs[:half], zs[half:]
    corr = dot(inv_ref[:taps, :], spectrum_of(gr * zr + gi * zi, gi * zr - gr * zi))
    share = corr_ref.shape[2]
    for part in range(corr_ref.shape[0]):
        corr_ref[part] = corr[:, part * share : (part + 1) * share]


def medium_kernel(z_ref, tail_ref, up_ref, f_ref, skip_ref, fz_ref, fh_ref, inv_ref, gq_ref):
    rows, _ = up_ref.shape
    half = fz_ref.shape[0] // 2
    zs = dot(fz_ref[...], jnp.concatenate([tail_ref[...], z_ref[...]], 0))
    hs = dot(fh_ref[...], f_ref[...].astype(BF16))
    hr, hi = hs[:half] + skip_ref[...], hs[half:]
    zr, zi = zs[:half], zs[half:]
    conv = dot(inv_ref[:rows, :], spectrum_of(zr * hr - zi * hi, zr * hi + zi * hr))
    gq_ref[...] = (up_ref[...].astype(F32) * conv).astype(BF16)


def back_kernel(width, nsq, *refs):
    scale_ref, ws = refs[0], refs[1 : 1 + nsq]
    (q_ref, k_ref, v_ref, tail_ref, head_ref, conv_ref, gn_ref, gain_ref, f_ref,
     gq_ref, gk_ref, gv_ref, small_ref, pad_p, pad_g, coef_ref) = refs[1 + nsq :]
    rows, block = q_ref.shape
    halo = tail_ref.shape[0]
    taps = f_ref.shape[0]
    share = small_ref.shape[2]

    @pl.when(pl.program_id(0) == 0)
    def _():
        scale = scale_ref[...]
        weight = ws[0][...]
        for part in ws[1:]:
            weight = weight + part[...]
        coef = jnp.sum(weight, axis=1, keepdims=True) * (scale * scale * scale) * (1.0 / width)
        coef_ref[...] = coef

    scale, coef = scale_ref[...], coef_ref[...]
    for start in range(0, block, LANES):
        cols = slice(start, start + LANES)
        q = q_ref[:, cols].astype(F32)
        conv = conv_ref[:, cols]
        mixed = q * conv
        gn = gn_ref[:, cols] * scale
        gm = gain_ref[:, cols] * gn - mixed * coef
        gq_ref[:, cols] = (gm * conv).astype(BF16)
        gc = (gm * q).astype(BF16).astype(F32)
        pad_g[:rows, :] = gc
        pad_g[rows:, :] = head_ref[:, cols].astype(F32)
        part, inner = start // share, start % share
        place = slice(inner, inner + LANES)
        small_ref[part, taps : taps + 1, place] = jnp.sum(gn * mixed, axis=0, keepdims=True)
        k = k_ref[:, cols].astype(F32)
        v = v_ref[:, cols].astype(F32)
        pad_p[:halo, :] = tail_ref[:, cols].astype(F32)
        pad_p[halo:, :] = (k * v).astype(BF16).astype(F32)
        gp = f_ref[0:1, cols] * gc
        for j in range(taps):
            if j:
                gp = gp + f_ref[j : j + 1, cols] * pad_g[pl.ds(j, rows), :]
            small_ref[part, j : j + 1, place] = jnp.sum(
                gc * pad_p[pl.ds(halo - j, rows), :], axis=0, keepdims=True
            )
        gk_ref[:, cols] = (gp * v).astype(BF16)
        gv_ref[:, cols] = (gp * k).astype(BF16)


def up_to(value, step):
    return -(-value // step) * step


def split_parts(parts, share):
    count, height, group = parts.shape
    if group == share:
        return parts
    parts = parts.reshape(count, height, group // share, share)
    return parts.transpose(0, 2, 1, 3).reshape(-1, height, share)


def scatter_sum(parts, axis):
    size = lax.axis_size(axis)
    me = lax.axis_index(axis)
    bit = 1
    while bit < size:
        rest = parts.reshape((parts.shape[0] // 2, 2) + parts.shape[1:])
        mine = lax.rem(me // bit, 2)
        away = lax.dynamic_index_in_dim(rest, 1 - mine, 1, keepdims=False).astype(BF16)
        keep = lax.dynamic_index_in_dim(rest, mine, 1, keepdims=False)
        got = lax.ppermute(away, axis, [(i, i ^ bit) for i in range(size)])
        parts = keep + got.astype(F32)
        bit *= 2
    return parts[0]


def exchanged(value, axis):
    size = lax.axis_size(axis)
    others = []
    for step in range(1, size):
        others.append(lax.ppermute(value, axis, [(i, (i + step) % size) for i in range(size)]))
    return [value] + others


def local(
    query_se, key_se, value_se, query_mr, key_mr, upstream, filter_se, filter_mr, skip_mr, norm_gain
):
    rows, chans = query_se.shape
    taps_se, taps = filter_se.shape[0], filter_mr.shape[0]
    ctx = lax.axis_size("ctx")
    width = chans * lax.axis_size("tp")
    tokens = rows * ctx
    share = chans // ctx
    group = up_to(share, LANES)
    halo = up_to(taps_se - 1, 16)
    block = max(group, min(512, chans))
    steps = chans // block
    fz, fg, fh, inv = transforms(rows, taps)
    length = rows + taps
    skip = skip_mr[None]
    gain = norm_gain[None]

    def rowed(n):
        return pl.BlockSpec((n, block), lambda i: (0, i))

    def whole(a):
        return pl.BlockSpec(a.shape, lambda i: (0, 0))

    lanes_spec = pl.BlockSpec((rows, LANES), lambda i: (0, 0))
    stream = rowed(rows)
    one = rowed(1)

    def call(body, ins, specs, outs, out_specs, scratch=(), flops=0):
        moved = sum(a.size * a.dtype.itemsize for a in list(ins) + list(outs))
        return pl.pallas_call(
            body,
            grid=(steps,),
            in_specs=specs,
            out_specs=out_specs,
            out_shape=outs,
            scratch_shapes=scratch,
            cost_estimate=pl.CostEstimate(flops=flops, bytes_accessed=moved, transcendentals=0),
            compiler_params=pltpu.CompilerParams(
                dimension_semantics=("arbitrary",), vmem_limit_bytes=58 * 2**20
            ),
        )(*ins)

    def shape(n, kind):
        return jax.ShapeDtypeStruct((n, chans), kind)

    lanes_shape = jax.ShapeDtypeStruct((rows, LANES), F32)

    tail_se = shifted(
        (key_se[rows - halo :].astype(F32) * value_se[rows - halo :].astype(F32)).astype(BF16),
        "ctx", 1,
    )
    head_mr = shifted(
        (upstream[:taps].astype(F32) * query_mr[:taps].astype(F32)).astype(BF16), "ctx", -1
    )
    conv_se, squares = call(
        short_kernel,
        (query_se, key_se, value_se, tail_se, filter_se),
        [stream, stream, stream, rowed(halo), rowed(taps_se)],
        [shape(rows, F32), lanes_shape], [stream, lanes_spec],
        [pltpu.VMEM((halo + rows, LANES), F32)],
    )
    sq = exchanged(squares, "tp")
    nsq = len(sq)
    group_spec = pl.BlockSpec((block // group, taps, group), lambda i: (i, 0, 0))
    grad_key_mr, grad_normed, weight, product_mr, tail, corr, scales = call(
        functools.partial(adjoint_kernel, width, nsq),
        (*sq, upstream, query_mr, head_mr, filter_mr, skip, query_se, conv_se, key_mr, gain,
         fg, fh, inv),
        [lanes_spec] * nsq
        + [stream, stream, rowed(taps), rowed(taps), one, stream, stream, stream, one,
           whole(fg), whole(fh), whole(inv)],
        [shape(rows, BF16), shape(rows, F32), lanes_shape, shape(rows, BF16),
         shape(taps, BF16), jax.ShapeDtypeStruct((chans // group, taps, group), F32),
         lanes_shape],
        [stream, stream, lanes_spec, stream, rowed(taps), group_spec, lanes_spec],
        flops=2 * length * (length + taps + 2 * rows + taps) * chans,
    )
    tail_mr = shifted(tail, "ctx", 1)
    ws = exchanged(weight, "tp")
    first = slice(0, halo)
    scale = scales[first, :1]
    coef = scale**3 * jnp.sum(sum(a[first] for a in ws), axis=1, keepdims=True) / width
    q_head = query_se[first].astype(F32)
    mixed_head = gain * scale * grad_normed[first] - q_head * conv_se[first] * coef
    head_send = (mixed_head * q_head).astype(BF16)
    head_se = shifted(head_send, "ctx", -1)
    grad_query_se, grad_key_se, grad_value_se, small = call(
        functools.partial(back_kernel, width, nsq),
        (scales, *ws, query_se, key_se, value_se, tail_se, head_se, conv_se, grad_normed, gain,
         filter_se),
        [lanes_spec] * (1 + nsq)
        + [stream, stream, stream, rowed(halo), rowed(halo), stream, stream, one, rowed(taps_se)],
        [shape(rows, BF16)] * 3 + [jax.ShapeDtypeStruct((chans // group, taps_se + 1, group), F32)],
        [stream] * 3 + [pl.BlockSpec((block // group, taps_se + 1, group), lambda i: (i, 0, 0))],
        [pltpu.VMEM((halo + rows, LANES), F32)] * 2 + [pltpu.VMEM((rows, LANES), F32)],
    )
    corr, small = split_parts(corr, share), split_parts(small, share)
    small = lax.all_to_all(small, "ctx", 0, 0, tiled=True)
    (grad_query_mr,) = call(
        medium_kernel,
        (product_mr, tail_mr, upstream, filter_mr, skip, fz, fh, inv),
        [stream, rowed(taps), stream, rowed(taps), one, whole(fz), whole(fh), whole(inv)],
        [shape(rows, BF16)], [stream],
        flops=2 * length * (length + taps + rows) * chans,
    )
    factor = 1.0 / math.sqrt(tokens)
    total_mr = scatter_sum(corr, "ctx") * factor
    total = jnp.sum(small, axis=0) * factor
    return (
        grad_query_se,
        grad_key_se,
        grad_value_se,
        grad_query_mr,
        grad_key_mr,
        total[:taps_se],
        total_mr,
        total_mr[0],
        total[taps_se],
    )


def solution(mesh):
    streams = (P("ctx", "tp"),)
    in_specs = streams * 6 + (P(None, "tp"), P(None, "tp"), P("tp"), P("tp"))
    both = ("tp", "ctx")
    out_specs = streams * 5 + (P(None, both), P(None, both), P(both), P(both))

    return jax.shard_map(local, mesh=mesh, in_specs=in_specs, out_specs=out_specs, check_vma=False)
```

```python
import functools
import math

import jax
import jax.numpy as jnp
import numpy as np
from jax import lax
from jax.experimental import pallas as pl
from jax.experimental.pallas import tpu as pltpu
from jax.sharding import PartitionSpec as P


EPSILON = 0.1
F32 = jnp.float32
BF16 = jnp.bfloat16
LANES = 128


def shifted(block, axis, distance):
    devices = range(lax.axis_size(axis))
    route = [(i - distance, i) for i in devices if i - distance in devices]
    return lax.ppermute(block, axis, route)


def transforms(rows, taps):
    length = rows + taps
    freq = 2.0 * np.pi * (np.arange(length // 2) + 0.5) / length

    def forward(start, stop):
        angle = freq[:, None] * np.arange(start, stop)[None, :]
        return np.concatenate([np.cos(angle), -np.sin(angle)], 0)

    angle = np.arange(max(rows, taps))[:, None] * freq[None, :]
    inverse = np.concatenate([np.cos(angle), -np.sin(angle)], 1) * (2.0 / length)
    mats = forward(-taps, rows), forward(0, length), forward(0, taps), inverse
    return [jnp.asarray(m, BF16) for m in mats]


def dot(a, b):
    return jnp.dot(a, b, preferred_element_type=F32)


def row_scale(width, *parts):
    total = parts[0][...]
    for part in parts[1:]:
        total = total + part[...]
    return lax.rsqrt(jnp.sum(total, axis=1, keepdims=True) * (1.0 / width) + EPSILON)


def short_kernel(q_ref, k_ref, v_ref, tail_ref, f_ref, conv_ref, sq_ref, pad):
    rows, block = q_ref.shape
    halo = tail_ref.shape[0]

    @pl.when(pl.program_id(0) == 0)
    def _():
        sq_ref[...] = jnp.zeros_like(sq_ref)

    for start in range(0, block, LANES):
        cols = slice(start, start + LANES)
        pad[:halo, cols] = tail_ref[:, cols].astype(F32)
        product = k_ref[:, cols].astype(F32) * v_ref[:, cols].astype(F32)
        pad[halo:, cols] = product.astype(BF16).astype(F32)
        conv = f_ref[0:1, cols] * pad[pl.ds(halo, rows), cols]
        for j in range(1, f_ref.shape[0]):
            conv = conv + f_ref[j : j + 1, cols] * pad[pl.ds(halo - j, rows), cols]
        conv_ref[:, cols] = conv
        mixed = q_ref[:, cols].astype(F32) * conv
        sq_ref[...] += mixed * mixed


def spectrum_of(real, imag):
    return jnp.concatenate([real.astype(BF16), imag.astype(BF16)], 0)


def adjoint_kernel(width, nsq, *refs):
    sq = refs[:nsq]
    (up_ref, qm_ref, head_ref, f_ref, skip_ref, q_ref, conv_ref, km_ref, gain_ref,
     fg_ref, fh_ref, inv_ref, gk_ref, gn_ref, w_ref, z_ref, tail_ref, corr_ref,
     scale_ref) = refs[nsq:]
    rows, block = q_ref.shape
    taps = f_ref.shape[0]
    half = fg_ref.shape[0] // 2

    @pl.when(pl.program_id(0) == 0)
    def _():
        w_ref[...] = jnp.zeros_like(w_ref)
        scale_ref[...] = jnp.broadcast_to(row_scale(width, *sq), scale_ref.shape)

    g = (up_ref[...].astype(F32) * qm_ref[...].astype(F32)).astype(BF16)
    gs = dot(fg_ref[...], jnp.concatenate([g, head_ref[...]], 0))
    hs = dot(fh_ref[...], f_ref[...].astype(BF16))
    hr, hi = hs[:half] + skip_ref[...], hs[half:]
    gr, gi = gs[:half], gs[half:]
    gp = dot(inv_ref[:rows, :], spectrum_of(gr * hr + gi * hi, gi * hr - gr * hi))
    scale = scale_ref[...]
    for start in range(0, block, LANES):
        cols = slice(start, start + LANES)
        mixed = q_ref[:, cols].astype(F32) * conv_ref[:, cols]
        back = gp[:, cols]
        gain = gain_ref[:, cols]
        km = km_ref[:, cols].astype(F32)
        normed = mixed * scale * gain
        gk_ref[:, cols] = (back * normed).astype(BF16)
        z_ref[:, cols] = (km * normed).astype(BF16)
        gn = back * km
        gn_ref[:, cols] = gn
        w_ref[...] += gn * gain * mixed
    tail_ref[...] = z_ref[rows - taps :, :]
    zs = dot(fg_ref[:, :rows], z_ref[...])
    zr, zi = zs[:half], zs[half:]
    corr = dot(inv_ref[:taps, :], spectrum_of(gr * zr + gi * zi, gi * zr - gr * zi))
    share = corr_ref.shape[2]
    for part in range(corr_ref.shape[0]):
        corr_ref[part] = corr[:, part * share : (part + 1) * share]


def medium_kernel(z_ref, tail_ref, up_ref, f_ref, skip_ref, fz_ref, fh_ref, inv_ref, gq_ref):
    rows, _ = up_ref.shape
    half = fz_ref.shape[0] // 2
    zs = dot(fz_ref[...], jnp.concatenate([tail_ref[...], z_ref[...]], 0))
    hs = dot(fh_ref[...], f_ref[...].astype(BF16))
    hr, hi = hs[:half] + skip_ref[...], hs[half:]
    zr, zi = zs[:half], zs[half:]
    conv = dot(inv_ref[:rows, :], spectrum_of(zr * hr - zi * hi, zr * hi + zi * hr))
    gq_ref[...] = (up_ref[...].astype(F32) * conv).astype(BF16)


def back_kernel(width, nsq, *refs):
    scale_ref, ws = refs[0], refs[1 : 1 + nsq]
    (q_ref, k_ref, v_ref, tail_ref, head_ref, conv_ref, gn_ref, gain_ref, f_ref,
     gq_ref, gk_ref, gv_ref, small_ref, pad_p, pad_g, coef_ref) = refs[1 + nsq :]
    rows, block = q_ref.shape
    halo = tail_ref.shape[0]
    taps = f_ref.shape[0]
    share = small_ref.shape[2]

    @pl.when(pl.program_id(0) == 0)
    def _():
        scale = scale_ref[...]
        weight = ws[0][...]
        for part in ws[1:]:
            weight = weight + part[...]
        coef = jnp.sum(weight, axis=1, keepdims=True) * (scale * scale * scale) * (1.0 / width)
        coef_ref[...] = coef

    scale, coef = scale_ref[...], coef_ref[...]
    for start in range(0, block, LANES):
        cols = slice(start, start + LANES)
        q = q_ref[:, cols].astype(F32)
        conv = conv_ref[:, cols]
        mixed = q * conv
        gn = gn_ref[:, cols] * scale
        gm = gain_ref[:, cols] * gn - mixed * coef
        gq_ref[:, cols] = (gm * conv).astype(BF16)
        gc = (gm * q).astype(BF16).astype(F32)
        pad_g[:rows, cols] = gc
        pad_g[rows:, cols] = head_ref[:, cols].astype(F32)
        part, inner = start // share, start % share
        place = slice(inner, inner + LANES)
        small_ref[part, taps : taps + 1, place] = jnp.sum(gn * mixed, axis=0, keepdims=True)
        k = k_ref[:, cols].astype(F32)
        v = v_ref[:, cols].astype(F32)
        pad_p[:halo, cols] = tail_ref[:, cols].astype(F32)
        pad_p[halo:, cols] = (k * v).astype(BF16).astype(F32)
        gp = f_ref[0:1, cols] * gc
        for j in range(taps):
            if j:
                gp = gp + f_ref[j : j + 1, cols] * pad_g[pl.ds(j, rows), cols]
            small_ref[part, j : j + 1, place] = jnp.sum(
                gc * pad_p[pl.ds(halo - j, rows), cols], axis=0, keepdims=True
            )
        gk_ref[:, cols] = (gp * v).astype(BF16)
        gv_ref[:, cols] = (gp * k).astype(BF16)


def up_to(value, step):
    return -(-value // step) * step


def split_parts(parts, share):
    count, height, group = parts.shape
    if group == share:
        return parts
    parts = parts.reshape(count, height, group // share, share)
    return parts.transpose(0, 2, 1, 3).reshape(-1, height, share)


def scatter_sum(parts, axis):
    size = lax.axis_size(axis)
    me = lax.axis_index(axis)
    bit = 1
    while bit < size:
        rest = parts.reshape((parts.shape[0] // 2, 2) + parts.shape[1:])
        mine = lax.rem(me // bit, 2)
        away = lax.dynamic_index_in_dim(rest, 1 - mine, 1, keepdims=False).astype(BF16)
        keep = lax.dynamic_index_in_dim(rest, mine, 1, keepdims=False)
        got = lax.ppermute(away, axis, [(i, i ^ bit) for i in range(size)])
        parts = keep + got.astype(F32)
        bit *= 2
    return parts[0]


def exchanged(value, axis):
    size = lax.axis_size(axis)
    others = []
    for step in range(1, size):
        others.append(lax.ppermute(value, axis, [(i, (i + step) % size) for i in range(size)]))
    return [value] + others


def local(
    query_se, key_se, value_se, query_mr, key_mr, upstream, filter_se, filter_mr, skip_mr, norm_gain
):
    rows, chans = query_se.shape
    taps_se, taps = filter_se.shape[0], filter_mr.shape[0]
    ctx = lax.axis_size("ctx")
    width = chans * lax.axis_size("tp")
    tokens = rows * ctx
    share = chans // ctx
    group = up_to(share, LANES)
    halo = up_to(taps_se - 1, 16)
    block = max(group, min(512, chans))
    steps = chans // block
    fz, fg, fh, inv = transforms(rows, taps)
    length = rows + taps
    skip = skip_mr[None]
    gain = norm_gain[None]

    def rowed(n):
        return pl.BlockSpec((n, block), lambda i: (0, i))

    def whole(a):
        return pl.BlockSpec(a.shape, lambda i: (0, 0))

    lanes_spec = pl.BlockSpec((rows, LANES), lambda i: (0, 0))
    stream = rowed(rows)
    one = rowed(1)

    def call(body, ins, specs, outs, out_specs, scratch=(), flops=0):
        moved = sum(a.size * a.dtype.itemsize for a in list(ins) + list(outs))
        return pl.pallas_call(
            body,
            grid=(steps,),
            in_specs=specs,
            out_specs=out_specs,
            out_shape=outs,
            scratch_shapes=scratch,
            cost_estimate=pl.CostEstimate(flops=flops, bytes_accessed=moved, transcendentals=0),
            compiler_params=pltpu.CompilerParams(
                dimension_semantics=("arbitrary",), vmem_limit_bytes=58 * 2**20
            ),
        )(*ins)

    def shape(n, kind):
        return jax.ShapeDtypeStruct((n, chans), kind)

    lanes_shape = jax.ShapeDtypeStruct((rows, LANES), F32)

    tail_se = shifted(
        (key_se[rows - halo :].astype(F32) * value_se[rows - halo :].astype(F32)).astype(BF16),
        "ctx", 1,
    )
    head_mr = shifted(
        (upstream[:taps].astype(F32) * query_mr[:taps].astype(F32)).astype(BF16), "ctx", -1
    )
    conv_se, squares = call(
        short_kernel,
        (query_se, key_se, value_se, tail_se, filter_se),
        [stream, stream, stream, rowed(halo), rowed(taps_se)],
        [shape(rows, F32), lanes_shape], [stream, lanes_spec],
        [pltpu.VMEM((halo + rows, block), F32)],
    )
    sq = exchanged(squares, "tp")
    nsq = len(sq)
    group_spec = pl.BlockSpec((block // group, taps, group), lambda i: (i, 0, 0))
    grad_key_mr, grad_normed, weight, product_mr, tail, corr, scales = call(
        functools.partial(adjoint_kernel, width, nsq),
        (*sq, upstream, query_mr, head_mr, filter_mr, skip, query_se, conv_se, key_mr, gain,
         fg, fh, inv),
        [lanes_spec] * nsq
        + [stream, stream, rowed(taps), rowed(taps), one, stream, stream, stream, one,
           whole(fg), whole(fh), whole(inv)],
        [shape(rows, BF16), shape(rows, F32), lanes_shape, shape(rows, BF16),
         shape(taps, BF16), jax.ShapeDtypeStruct((chans // group, taps, group), F32),
         lanes_shape],
        [stream, stream, lanes_spec, stream, rowed(taps), group_spec, lanes_spec],
        flops=2 * length * (length + taps + 2 * rows + taps) * chans,
    )
    tail_mr = shifted(tail, "ctx", 1)
    ws = exchanged(weight, "tp")
    first = slice(0, halo)
    scale = scales[first, :1]
    coef = scale**3 * jnp.sum(sum(a[first] for a in ws), axis=1, keepdims=True) / width
    q_head = query_se[first].astype(F32)
    mixed_head = gain * scale * grad_normed[first] - q_head * conv_se[first] * coef
    head_send = (mixed_head * q_head).astype(BF16)
    head_se = shifted(head_send, "ctx", -1)
    grad_query_se, grad_key_se, grad_value_se, small = call(
        functools.partial(back_kernel, width, nsq),
        (scales, *ws, query_se, key_se, value_se, tail_se, head_se, conv_se, grad_normed, gain,
         filter_se),
        [lanes_spec] * (1 + nsq)
        + [stream, stream, stream, rowed(halo), rowed(halo), stream, stream, one, rowed(taps_se)],
        [shape(rows, BF16)] * 3 + [jax.ShapeDtypeStruct((chans // group, taps_se + 1, group), F32)],
        [stream] * 3 + [pl.BlockSpec((block // group, taps_se + 1, group), lambda i: (i, 0, 0))],
        [pltpu.VMEM((halo + rows, block), F32)] * 2 + [pltpu.VMEM((rows, LANES), F32)],
    )
    corr, small = split_parts(corr, share), split_parts(small, share)
    small = lax.all_to_all(small, "ctx", 0, 0, tiled=True)
    (grad_query_mr,) = call(
        medium_kernel,
        (product_mr, tail_mr, upstream, filter_mr, skip, fz, fh, inv),
        [stream, rowed(taps), stream, rowed(taps), one, whole(fz), whole(fh), whole(inv)],
        [shape(rows, BF16)], [stream],
        flops=2 * length * (length + taps + rows) * chans,
    )
    factor = 1.0 / math.sqrt(tokens)
    total_mr = scatter_sum(corr, "ctx") * factor
    total = jnp.sum(small, axis=0) * factor
    return (
        grad_query_se,
        grad_key_se,
        grad_value_se,
        grad_query_mr,
        grad_key_mr,
        total[:taps_se],
        total_mr,
        total_mr[0],
        total[taps_se],
    )


def solution(mesh):
    streams = (P("ctx", "tp"),)
    in_specs = streams * 6 + (P(None, "tp"), P(None, "tp"), P("tp"), P("tp"))
    both = ("tp", "ctx")
    out_specs = streams * 5 + (P(None, both), P(None, both), P(both), P(both))

    return jax.shard_map(local, mesh=mesh, in_specs=in_specs, out_specs=out_specs, check_vma=False)
```
